32 devices in a mesh: pole: 2 (over y), leaf: 16 (over z, x, core).
Axes of the slice: x: 2, y: 2, z: 4, core: 2. Of those that a mesh axis runs over, the one named last changes fastest.
Arguments:
- root_frame: float32 [2048, 1024], P(('pole', 'leaf')), parts along dimension 0, may hold values from -2 to 8, as said below
- top_lhat: float32 [3072, 256], P(('pole', 'leaf')), parts along dimension 0, may hold values from -0.21875 to 0.21875
- top_dinv: float32 [1024, 256], P(('pole', 'leaf')), parts along dimension 0, may hold values from -2 to 8, as said below
- mid_lhat: float32 [32, 768, 256], P(('pole', 'leaf')), parts along dimension 0, may hold values from -0.21875 to 0.21875
- mid_dinv: float32 [32, 256, 256], P(('pole', 'leaf')), parts along dimension 0, may hold values from -2 to 8, as said below
- leaf_lhat: float32 [64, 768, 256], P(('pole', 'leaf')), parts along dimension 0, may hold values from -0.21875 to 0.21875
- leaf_dinv: float32 [64, 256, 256], P(('pole', 'leaf')), parts along dimension 0, may hold values from -2 to 8, as said below
- top_columns: int32 [2], replicated, may hold values from 128 to 256
- mid_columns: int32 [16], replicated, may hold values from 128 to 256
- leaf_columns: int32 [32], replicated, may hold values from 128 to 256
- top_pattern: int32 [2, 3], replicated, may hold values from 0 to 3, as said below
- mid_parent: int32 [16], replicated, may hold values from 0 to 1, as said below
- leaf_parent: int32 [32], replicated, may hold values from 0 to 15, as said below
- mid_pattern: int32 [16, 3], replicated, may hold values from 0 to 3, as said below
- leaf_pattern: int32 [32, 3], replicated, may hold values from 0 to 3, as said below
- leaf_live: int32 [16], replicated, may hold values from 1 to 2, as said below
Outputs:
- top_diagonal: float32 [1024, 256], P(('pole', 'leaf')), parts along dimension 0
- top_coupling: float32 [3072, 256], P(('pole', 'leaf')), parts along dimension 0
- mid_diagonal: float32 [32, 256, 256], P(('pole', 'leaf')), parts along dimension 0
- mid_coupling: float32 [32, 768, 256], P(('pole', 'leaf')), parts along dimension 0
- leaf_diagonal: float32 [64, 256, 256], P(('pole', 'leaf')), parts along dimension 0
- leaf_coupling: float32 [64, 768, 256], P(('pole', 'leaf')), parts along dimension 0
The draws below stay inside these ranges and needn't reach their ends.
There are 2 independent parts, one for each index of `pole`. The reference program is written for one: setup_inputs(seed, part) draws one part's arguments, and reference() takes and returns one part's arrays. A program takes and returns all parts, laid end to end along the dimension named above; an argument that names none is the same for every part. Nothing has to cross between parts.
Inputs may be any that keep to these rules, and one draw needn't show every extreme that they name: `root_frame`: Symmetric. `top_dinv`: each 256 x 256 block is symmetric. `mid_dinv`: each block is symmetric. `leaf_dinv`: each block is symmetric. `top_pattern`: each row holds 3 distinct increasing numbers of 0 to 3. mid_parent[j] is 2 * (j // 16) plus a number below 2: a level-1 supernode hangs under a level-2 supernode of its own group of 16 devices. leaf_parent[i] is one of the 4 level-1 supernodes numbered from 4 * (i // 8): a leaf hangs under a level-1 supernode of its own group of 4 devices. `mid_pattern`: each row starts with 0 (the parent) and goes on with 2 distinct increasing numbers of 1 to 3. `leaf_pattern`: each row starts with 0 (the parent) and goes on with 2 distinct increasing numbers of 1 to 3. The leaf supernodes of device d are its first leaf_live[d] slots; some device has all 2.
All inputs are finite; a program needn't handle non-finite values.
Results may differ from the reference program's by a relative error of at most 0.0003.
Values sent between devices are 32-bit elements; how exact they have to be, the bound alone decides.
No kernel may reach another device: no remote copies, remote signals or barrier semaphores. Data moves between devices by JAX's collectives and lax.ppermute only.
A program may use at most 128 MiB of HBM per device.

```python
import jax
import jax.numpy as jnp
from jax import lax

COLS = 256
SLOTS = 3
GROUP2 = 16
NODES2 = 2
GROUP1 = 4
L0_DEV = 2
ROOTB = 4
TOP = 2
MID = 16
LEAFS = 32


def symmetric_blocks(key, number, extent):
    noise_key, scale_key = jax.random.split(key)
    noise = jax.random.normal(noise_key, (number, extent, extent), jnp.float32)
    diagonal = jax.random.uniform(scale_key, (number, extent), jnp.float32, 1.0, 3.0)
    twin = (noise + jnp.swapaxes(noise, 1, 2)) * (0.45 / jnp.sqrt(extent * 1.0))
    return twin + diagonal[:, :, None] * jnp.eye(extent, dtype=jnp.float32)[None]


def draw_root_frame(key, part):
    blocks = symmetric_blocks(jax.random.fold_in(key, 11), 1, ROOTB * COLS)
    return blocks.reshape(ROOTB * COLS, ROOTB * COLS)


def draw_top_dinv(key, part):
    blocks = symmetric_blocks(jax.random.fold_in(key, 12), TOP, COLS)
    return blocks.reshape(TOP * COLS, COLS)


def draw_mid_dinv(key, part):
    return symmetric_blocks(jax.random.fold_in(key, 13), MID, COLS)


def draw_leaf_dinv(key, part):
    return symmetric_blocks(jax.random.fold_in(key, 14), LEAFS, COLS)


def draw_top_pattern(key, part):
    skipped = jax.random.randint(jax.random.fold_in(key, 33), (TOP, 1), 0, SLOTS + 1)
    later = jnp.arange(0, SLOTS, dtype=jnp.int32)[None, :]
    return (later + (later >= skipped).astype(jnp.int32)).astype(jnp.int32)


def draw_mid_parent(key, part):
    offsets = jax.random.randint(jax.random.fold_in(key, 21), (MID,), 0, NODES2)
    return (jnp.arange(MID, dtype=jnp.int32) // GROUP2 * NODES2 + offsets).astype(jnp.int32)


def draw_leaf_parent(key, part):
    holder = jnp.arange(LEAFS, dtype=jnp.int32) // L0_DEV
    offsets = jax.random.randint(jax.random.fold_in(key, 22), (LEAFS,), 0, GROUP1)
    return (holder // GROUP1 * GROUP1 + offsets).astype(jnp.int32)


def pattern_rows(key, number):
    skipped = jax.random.randint(key, (number, 1), 1, SLOTS + 1)
    later = jnp.arange(1, SLOTS, dtype=jnp.int32)[None, :]
    remaining = later + (later >= skipped).astype(jnp.int32)
    return jnp.concatenate([jnp.zeros((number, 1), jnp.int32), remaining], axis=1).astype(jnp.int32)


def draw_mid_pattern(key, part):
    return pattern_rows(jax.random.fold_in(key, 31), MID)


def draw_leaf_pattern(key, part):
    return pattern_rows(jax.random.fold_in(key, 32), LEAFS)


def draw_leaf_live(key, part):
    first_key, second_key, peak_key = jax.random.split(jax.random.fold_in(key, 41), 3)
    lower_count = jnp.minimum(jax.random.randint(first_key, (MID,), 0, L0_DEV), jax.random.randint(second_key, (MID,), 0, L0_DEV)) + 1
    peak_device = jax.random.randint(peak_key, (), 0, MID)
    return jnp.where(jnp.arange(MID, dtype=jnp.int32) == peak_device, L0_DEV, lower_count).astype(jnp.int32)


def with_ends(array, rng, least, high):
    dims = array.shape
    place = [jax.random.randint(jax.random.fold_in(rng, axis), (), 0, dims[axis]) for axis in range(len(dims))]
    array = array.at[tuple(place)].set(least)
    longest = dims.index(max(dims))
    place[longest] = (place[longest] + 1) % dims[longest]
    return array.at[tuple(place)].set(high)


def level_of(rng, shape, cuts, low, top_value):
    loudness = 1.0
    for position, shards_of in cuts:
        draws = jax.random.uniform(jax.random.fold_in(jax.random.fold_in(rng, 6), position), (shards_of,), jnp.float32, low / len(cuts), top_value / len(cuts))
        loudness = loudness * jnp.repeat(jnp.exp(draws), shape[position] // shards_of).reshape((-1,) + (1,) * (len(shape) - 1 - position))
    return loudness


def bell_draw(own_key, shape, scale, bound, shards=(), held_as=jnp.bfloat16):
    drawn = scale * jax.random.normal(own_key, shape, jnp.float32)
    if shards:
        drawn = drawn * level_of(own_key, shape, shards, -0.22, 0.18)
    return jnp.clip(drawn, -bound, bound).astype(held_as)


def setup_inputs(seed: int = 0, part: int = 0) -> dict:
    keys = jax.random.split(jax.random.key(seed), 17)
    part_splits = jax.random.split(jax.random.fold_in(keys[16], part), 17)
    root_frame = draw_root_frame(jax.random.fold_in(jax.random.fold_in(keys[16], part), 71), part)
    top_lhat = bell_draw(part_splits[1], (TOP * SLOTS * COLS, COLS), (SLOTS * COLS) ** -0.5, 0.21875, ((0, 16),), jnp.float32)
    top_dinv = draw_top_dinv(jax.random.fold_in(jax.random.fold_in(keys[16], part), 71), part)
    mid_lhat = bell_draw(part_splits[3], (MID, SLOTS * COLS, COLS), (SLOTS * COLS) ** -0.5, 0.21875, ((0, 16),), jnp.float32)
    mid_dinv = draw_mid_dinv(jax.random.fold_in(jax.random.fold_in(keys[16], part), 71), part)
    leaf_lhat = bell_draw(part_splits[5], (LEAFS, SLOTS * COLS, COLS), (SLOTS * COLS) ** -0.5, 0.21875, ((0, 16),), jnp.float32)
    leaf_dinv = draw_leaf_dinv(jax.random.fold_in(jax.random.fold_in(keys[16], part), 71), part)
    top_columns = jax.random.randint(keys[7], (TOP,), COLS // 2, COLS + 1).astype(jnp.int32)
    mid_columns = with_ends(jax.random.randint(keys[8], (MID,), COLS // 2, COLS + 1), jax.random.fold_in(keys[8], 1), COLS // 2, COLS).astype(jnp.int32)
    leaf_columns = with_ends(jax.random.randint(keys[9], (LEAFS,), COLS // 2, COLS + 1), jax.random.fold_in(keys[9], 1), COLS // 2, COLS).astype(jnp.int32)
    top_pattern = draw_top_pattern(jax.random.fold_in(keys[16], 71), part)
    mid_parent = draw_mid_parent(jax.random.fold_in(keys[16], 71), part)
    leaf_parent = draw_leaf_parent(jax.random.fold_in(keys[16], 71), part)
    mid_pattern = draw_mid_pattern(jax.random.fold_in(keys[16], 71), part)
    leaf_pattern = draw_leaf_pattern(jax.random.fold_in(keys[16], 71), part)
    leaf_live = draw_leaf_live(jax.random.fold_in(keys[16], 71), part)
    return dict(root_frame=root_frame, top_lhat=top_lhat, top_dinv=top_dinv, mid_lhat=mid_lhat, mid_dinv=mid_dinv, leaf_lhat=leaf_lhat, leaf_dinv=leaf_dinv, top_columns=top_columns, mid_columns=mid_columns, leaf_columns=leaf_columns, top_pattern=top_pattern, mid_parent=mid_parent, leaf_parent=leaf_parent, mid_pattern=mid_pattern, leaf_pattern=leaf_pattern, leaf_live=leaf_live)


highest = lax.Precision.HIGHEST


def masked_inputs(lhat_block, dinv_block, used_width):
    block_size = lhat_block.shape[-1]
    column_keep = (jnp.arange(block_size, dtype=jnp.int32) < used_width).astype(lhat_block.dtype)
    lhat_masked = lhat_block * column_keep[None, :]
    dinv_masked = dinv_block * column_keep[:, None] * column_keep[None, :]
    return lhat_masked, dinv_masked


def solve_node(local_frame, lhat_block, dinv_block, used_width):
    lhat_masked, dinv_masked = masked_inputs(lhat_block, dinv_block, used_width)
    coupling = -jnp.dot(local_frame, lhat_masked, precision=highest, preferred_element_type=jnp.float32)
    diagonal = dinv_masked - jnp.dot(lhat_masked.T, coupling, precision=highest, preferred_element_type=jnp.float32)
    return diagonal, coupling


def extended_matrix(diagonal, coupling, local_frame):
    upper_row = jnp.concatenate([diagonal, coupling.T], axis=1)
    lower_row = jnp.concatenate([coupling, local_frame], axis=1)
    return jnp.concatenate([upper_row, lower_row], axis=0)


def select_frame(matrix, pattern, block_size):
    row_ids = (pattern[:, None].astype(jnp.int32) * block_size + jnp.arange(block_size, dtype=jnp.int32)[None, :]).reshape(-1).astype(jnp.int32)
    picked = jnp.take(matrix, row_ids, axis=0)
    return jnp.take(picked, row_ids, axis=1)


def reference(root_frame, top_lhat, top_dinv, mid_lhat, mid_dinv, leaf_lhat, leaf_dinv, top_columns, mid_columns, leaf_columns, top_pattern, mid_parent, leaf_parent, mid_pattern, leaf_pattern, leaf_live):
    frame_size = SLOTS * COLS
    frame_nodes = lax.map(lambda pattern: select_frame(root_frame, pattern, COLS), top_pattern)
    lhat_nodes = top_lhat.reshape(TOP, frame_size, COLS)
    dinv_nodes = top_dinv.reshape(TOP, COLS, COLS)
    top_diag, top_coup = jax.vmap(solve_node)(frame_nodes, lhat_nodes, dinv_nodes, top_columns)
    upper_mats = jax.vmap(extended_matrix)(top_diag, top_coup, frame_nodes)

    def mid_one(node_index):
        parent = mid_parent[node_index]
        local_frame = select_frame(upper_mats[parent], mid_pattern[node_index], COLS)
        return solve_node(local_frame, mid_lhat[node_index], mid_dinv[node_index], mid_columns[node_index])

    mid_diag, mid_coup = lax.map(mid_one, jnp.arange(MID, dtype=jnp.int32))

    def leaf_one(node_index):
        parent = leaf_parent[node_index]
        above_frame = select_frame(upper_mats[mid_parent[parent]], mid_pattern[parent], COLS)
        matrix = extended_matrix(mid_diag[parent], mid_coup[parent], above_frame)
        local_frame = select_frame(matrix, leaf_pattern[node_index], COLS)
        diagonal, coupling = solve_node(local_frame, leaf_lhat[node_index], leaf_dinv[node_index], leaf_columns[node_index])
        live_mask = (node_index % L0_DEV < leaf_live[node_index // L0_DEV]).astype(diagonal.dtype)
        return diagonal * live_mask, coupling * live_mask

    leaf_diag, leaf_coup = lax.map(leaf_one, jnp.arange(LEAFS, dtype=jnp.int32))
    return (top_diag.reshape(TOP * COLS, COLS), top_coup.reshape(TOP * frame_size, COLS), mid_diag, mid_coup, leaf_diag, leaf_coup)
```

```python
import functools

import jax
import jax.numpy as jnp
from jax import lax
from jax.experimental import pallas as pl
from jax.experimental.pallas import tpu as pltpu
from jax.sharding import PartitionSpec as P

SLOTS = 3
GROUP2 = 16
NODES2 = 2
GROUP1 = 4
BLOCKS = SLOTS + 1
LAYERS = GROUP2 // GROUP1
PER_NODE = GROUP2 // NODES2


ROOT_POOL = BLOCKS * BLOCKS
NODE_POOL = 1 + 2 * SLOTS
TOP_POOL = ROOT_POOL
MID_POOL = TOP_POOL + NODES2 * NODE_POOL
POOL = MID_POOL + GROUP1 * NODE_POOL


def exchange(x, flip):
    pairs = [(i, i ^ flip) for i in range(lax.axis_size("leaf"))]
    return lax.ppermute(x, "leaf", pairs)


def exchange_inner(x):
    pairs = []
    for i in range(lax.axis_size("leaf")):
        layer = i % GROUP2 // GROUP1
        step = {1: GROUP1, 2: -GROUP1}.get(layer, 0)
        pairs.append((i, i + step))
    return lax.ppermute(x, "leaf", pairs)


def along_layers(own):
    outer_1 = exchange(own, GROUP1)
    inner_1 = exchange_inner(own)
    outer_2 = exchange(inner_1, GROUP1)
    inner_2 = exchange_inner(outer_1)
    outer_3 = exchange(inner_2, GROUP1)
    return [own, outer_1, inner_1, outer_2, inner_2, outer_3]


ARRIVAL = ((0, 1, 3, 5), (1, 0, 2, 4), (4, 2, 0, 1), (5, 3, 1, 0))


def pack_kernel(place, root, lhat, dinv, out):
    rows, width = root.shape
    block = width // BLOCKS
    half = block // 2
    row_block = place[0]
    right = place[1]
    for a in range(BLOCKS):

        @pl.when(row_block == a)
        def _():
            out[0:rows, :] = root[:, a * block : (a + 1) * block]
            b = (a + 1) % BLOCKS
            out[rows : 2 * rows, :] = root[:, b * block : (b + 1) * block]
            c = (a + 2) % BLOCKS
            low = root[:, c * block : c * block + half]
            high = root[:, c * block + half : (c + 1) * block]
            piece = jnp.where(right == 1, high, low)
            out[2 * rows : 2 * rows + rows // 2, 0:half] = piece[: rows // 2]
            out[2 * rows : 2 * rows + rows // 2, half:block] = piece[rows // 2 :]

    at = 2 * rows + rows // 2
    out[at : at + lhat.shape[0], :] = lhat[...]
    out[at + lhat.shape[0] :, :] = dinv[...]


def pack(place, root, lhat, dinv):
    rows = 2 * root.shape[0] + root.shape[0] // 2 + lhat.shape[0] + dinv.shape[0]
    vmem = pl.BlockSpec(memory_space=pltpu.VMEM)
    return pl.pallas_call(
        pack_kernel,
        out_shape=jax.ShapeDtypeStruct((rows, dinv.shape[1]), jnp.float32),
        in_specs=[pl.BlockSpec(memory_space=pltpu.SMEM), vmem, vmem, vmem],
        out_specs=vmem,
        compiler_params=pltpu.CompilerParams(vmem_limit_bytes=4 * 1024 * 1024),
        name="pack",
    )(place, root, lhat, dinv)


def split(x):
    high = x.astype(jnp.bfloat16)
    low = (x - high.astype(jnp.float32)).astype(jnp.bfloat16)
    return high, low


def dot(a, b):
    return jnp.dot(a, b, preferred_element_type=jnp.float32)


def solve_kernel(
    place,
    top_columns,
    mid_columns,
    leaf_columns,
    top_pattern,
    mid_parent,
    leaf_parent,
    mid_pattern,
    leaf_pattern,
    leaf_live,
    *refs,
    rows_root,
    rows_lhat,
    rows_dinv,
    leaves,
):
    kinds = 4
    arrays = 6
    pieces = [refs[k * arrays : (k + 1) * arrays] for k in range(kinds)]
    refs = refs[kinds * arrays :]
    mid_lhats = refs[0:4]
    mid_dinvs = refs[4:8]
    leaf_lhat, leaf_dinv = refs[8:10]
    o_top_diag, o_top_coup, o_mid_diag, o_mid_coup, o_leaf_diag, o_leaf_coup = refs[10:16]
    (
        gathered,
        high_pool,
        low_pool,
        lhat_mid,
        dinv_mid,
        lhat_leaf,
        dinv_leaf,
        lhat_high,
        lhat_low,
        turned_high,
        turned_low,
        top_coup,
        top_diag,
        mid_coup,
        mid_diag,
        leaf_coup,
        leaf_diag,
        piece_sems,
        mid_sems,
        leaf_sems,
        out_sems,
    ) = refs[16:]
    block = gathered.shape[-1]
    half = block // 2
    frame = SLOTS * block
    device = place[0]
    member = device % GROUP2
    layer = member // GROUP1
    inside = member % GROUP1
    top_base = device // GROUP2 * NODES2
    mid_base = device // GROUP1 * GROUP1

    for z in range(LAYERS):

        @pl.when(layer == z)
        def _():
            for kind in range(kinds):
                for y in range(LAYERS):
                    slot = y * GROUP1 + (inside ^ kind)
                    source = pieces[kind][ARRIVAL[z][y]]
                    pltpu.make_async_copy(source, gathered.at[slot], piece_sems.at[slot]).start()

    mid_copies = []
    for kind in range(GROUP1):
        slot = inside ^ kind
        mid_copies.append(
            pltpu.make_async_copy(mid_lhats[kind], lhat_mid.at[slot], mid_sems.at[0, kind])
        )
        mid_copies.append(
            pltpu.make_async_copy(mid_dinvs[kind], dinv_mid.at[slot], mid_sems.at[1, kind])
        )
    for copy in mid_copies:
        copy.start()
    leaf_copies = [
        pltpu.make_async_copy(leaf_lhat, lhat_leaf, leaf_sems.at[0]),
        pltpu.make_async_copy(leaf_dinv, dinv_leaf, leaf_sems.at[1]),
    ]
    for copy in leaf_copies:
        copy.start()
    for slot in range(GROUP2):
        pltpu.make_async_copy(pieces[0][0], gathered.at[slot], piece_sems.at[slot]).wait()

    def put(index, value):
        high, low = split(value)
        high_pool[index] = high
        low_pool[index] = low

    def put_root(a, b, value):
        put(a * BLOCKS + b, value)
        if a != b:
            put(b * BLOCKS + a, value.T)

    strips = block // rows_root

    def strip_rows(a, first, number):
        return jnp.concatenate(
            [gathered[a * strips + k, first : first + number, :] for k in range(strips)], axis=0
        )

    def quadrant(a, side):
        parts = []
        for k in range(side * strips // 2, (side + 1) * strips // 2):
            first = 2 * rows_root
            parts.append(gathered[a * strips + k, first : first + rows_root // 2, 0:half])
            parts.append(gathered[a * strips + k, first : first + rows_root // 2, half:block])
        return jnp.concatenate(parts, axis=0)

    for a in range(BLOCKS):
        put_root(a, a, strip_rows(a, 0, rows_root))
        put_root(a, (a + 1) % BLOCKS, strip_rows(a, rows_root, rows_root))
    for a in range(BLOCKS // 2):
        far = a + BLOCKS // 2
        upper = jnp.concatenate([quadrant(a, 0), quadrant(far, 1).T], axis=1)
        lower = jnp.concatenate([quadrant(far, 0).T, quadrant(a, 1)], axis=1)
        put_root(a, far, jnp.concatenate([upper, lower], axis=0))

    def solve(ids, lhat, dinv, used, coup_out, diag_out, pool_at):
        keep = lax.broadcasted_iota(jnp.int32, (1, block), 1) < used
        keep_rows = lax.broadcasted_iota(jnp.int32, (block, 1), 0) < used
        for v in range(SLOTS):
            rows = slice(v * block, (v + 1) * block)
            high, low = split(jnp.where(keep, lhat(v), 0.0))
            lhat_high[rows, :] = high
            lhat_low[rows, :] = low
        for u in range(SLOTS):
            rows = slice(u * block, (u + 1) * block)
            left_high = jnp.concatenate([high_pool[ids[u][v]] for v in range(SLOTS)], axis=1)
            left_low = jnp.concatenate([low_pool[ids[u][v]] for v in range(SLOTS)], axis=1)
            total = dot(left_high, lhat_high[...])
            total += dot(left_high, lhat_low[...])
            total += dot(left_low, lhat_high[...])
            coupling = -total
            coup_out[rows, :] = coupling
            turned = coupling.T
            high, low = split(turned)
            turned_high[:, rows] = high
            turned_low[:, rows] = low
            if pool_at is not None:
                put(pool_at + 1 + u, coupling)
                high_pool[pool_at + 1 + SLOTS + u] = high
                low_pool[pool_at + 1 + SLOTS + u] = low
        total = dot(turned_high[...], lhat_high[...])
        total += dot(turned_high[...], lhat_low[...])
        total += dot(turned_low[...], lhat_high[...])
        diagonal = jnp.where(keep & keep_rows, dinv, 0.0) - total
        diag_out[...] = diagonal
        if pool_at is not None:
            put(pool_at, diagonal)

    at_lhat = 2 * rows_root + rows_root // 2
    at_dinv = at_lhat + rows_lhat

    for q in range(NODES2):
        node = top_base + q
        pattern = [top_pattern[node, s] for s in range(SLOTS)]
        ids = [[pattern[u] * BLOCKS + pattern[v] for v in range(SLOTS)] for u in range(SLOTS)]

        def lhat_rows(v):
            parts = []
            first = v * block
            while first < (v + 1) * block:
                owner, offset = divmod(first, rows_lhat)
                number = min(rows_lhat - offset, (v + 1) * block - first)
                parts.append(
                    gathered[
                        q * PER_NODE + owner, at_lhat + offset : at_lhat + offset + number, :
                    ]
                )
                first += number
            return jnp.concatenate(parts, axis=0)

        dinv = jnp.concatenate(
            [
                gathered[q * PER_NODE + k, at_dinv : at_dinv + rows_dinv, :]
                for k in range(PER_NODE)
            ],
            axis=0,
        )
        solve(
            ids,
            lhat_rows,
            dinv,
            top_columns[node],
            top_coup.at[q],
            top_diag.at[q],
            TOP_POOL + q * NODE_POOL,
        )

    own_node = member // PER_NODE
    row_block = member % PER_NODE
    outs = [
        pltpu.make_async_copy(
            top_coup.at[own_node, pl.ds(row_block * rows_lhat, rows_lhat)],
            o_top_coup,
            out_sems.at[0],
        ),
        pltpu.make_async_copy(
            top_diag.at[own_node, pl.ds(row_block * rows_dinv, rows_dinv)],
            o_top_diag,
            out_sems.at[1],
        ),
    ]
    for copy in outs:
        copy.start()

    def frame_id(node, a, b):
        top = mid_parent[node] - top_base
        base = TOP_POOL + top * NODE_POOL
        slot_a = mid_pattern[node, a]
        slot_b = mid_pattern[node, b]
        above_a = jnp.maximum(slot_a - 1, 0)
        above_b = jnp.maximum(slot_b - 1, 0)
        inner = (
            top_pattern[top_base + top, above_a] * BLOCKS + top_pattern[top_base + top, above_b]
        )
        index = jnp.where(slot_a == 0, base + 1 + SLOTS + above_b, inner)
        index = jnp.where(slot_b == 0, base + 1 + above_a, index)
        return jnp.where((slot_a == 0) & (slot_b == 0), base, index)

    for copy in mid_copies + leaf_copies:
        copy.wait()

    live = leaf_live[device]

    @pl.loop(0, GROUP1)
    def _(number):
        node = mid_base + number
        needed = number == inside
        for leaf in range(leaves):
            used_here = leaf_parent[device * leaves + leaf] == node
            needed = needed | (used_here & (leaf < live))

        @pl.when(needed)
        def _():
            ids = [[frame_id(node, u, v) for v in range(SLOTS)] for u in range(SLOTS)]
            solve(
                ids,
                lambda v: lhat_mid[number, v * block : (v + 1) * block, :],
                dinv_mid[number],
                mid_columns[node],
                mid_coup.at[number],
                mid_diag.at[number],
                MID_POOL + number * NODE_POOL,
            )

    mid_outs = [
        pltpu.make_async_copy(mid_coup.at[inside], o_mid_coup, out_sems.at[2]),
        pltpu.make_async_copy(mid_diag.at[inside], o_mid_diag, out_sems.at[3]),
    ]
    for copy in mid_outs:
        copy.start()

    @pl.loop(0, leaves)
    def _(leaf):
        @pl.when(leaf < live)
        def _():
            node = device * leaves + leaf
            parent = leaf_parent[node]
            base = MID_POOL + (parent - mid_base) * NODE_POOL

            def leaf_id(u, v):
                slot_u = jnp.maximum(leaf_pattern[node, u] - 1, 0)
                slot_v = jnp.maximum(leaf_pattern[node, v] - 1, 0)
                if u == 0 and v == 0:
                    return base
                if u == 0:
                    return base + 1 + SLOTS + slot_v
                if v == 0:
                    return base + 1 + slot_u
                return frame_id(parent, slot_u, slot_v)

            ids = [[leaf_id(u, v) for v in range(SLOTS)] for u in range(SLOTS)]
            solve(
                ids,
                lambda v: lhat_leaf[leaf, v * block : (v + 1) * block, :],
                dinv_leaf[leaf],
                leaf_columns[node],
                leaf_coup.at[leaf],
                leaf_diag.at[leaf],
                None,
            )

        @pl.when(leaf >= live)
        def _():
            leaf_coup[leaf] = jnp.zeros((frame, block), jnp.float32)
            leaf_diag[leaf] = jnp.zeros((block, block), jnp.float32)

    leaf_outs = [
        pltpu.make_async_copy(leaf_coup, o_leaf_coup, out_sems.at[4]),
        pltpu.make_async_copy(leaf_diag, o_leaf_diag, out_sems.at[5]),
    ]
    for copy in leaf_outs:
        copy.start()
    for copy in outs + mid_outs + leaf_outs:
        copy.wait()


def solve_all(scalars, pieces, mids, leaf_lhat, leaf_dinv, rows):
    rows_root, rows_lhat, rows_dinv = rows
    leaves, frame, block = leaf_lhat.shape
    f32 = jnp.float32
    bf16 = jnp.bfloat16
    smem = pl.BlockSpec(memory_space=pltpu.SMEM)
    anywhere = pl.BlockSpec(memory_space=pl.ANY)
    arrays = [array for kind in pieces for array in kind]
    arrays += [mid[0] for mid in mids] + [mid[1] for mid in mids] + [leaf_lhat, leaf_dinv]
    return pl.pallas_call(
        functools.partial(
            solve_kernel,
            rows_root=rows_root,
            rows_lhat=rows_lhat,
            rows_dinv=rows_dinv,
            leaves=leaves,
        ),
        out_shape=(
            jax.ShapeDtypeStruct((rows_dinv, block), f32),
            jax.ShapeDtypeStruct((rows_lhat, block), f32),
            jax.ShapeDtypeStruct((block, block), f32),
            jax.ShapeDtypeStruct((frame, block), f32),
            jax.ShapeDtypeStruct((leaves, block, block), f32),
            jax.ShapeDtypeStruct((leaves, frame, block), f32),
        ),
        in_specs=[smem] * len(scalars) + [anywhere] * len(arrays),
        out_specs=(anywhere,) * 6,
        scratch_shapes=[
            pltpu.VMEM((GROUP2,) + pieces[0][0].shape, f32),
            pltpu.VMEM((POOL, block, block), bf16),
            pltpu.VMEM((POOL, block, block), bf16),
            pltpu.VMEM((GROUP1, frame, block), f32),
            pltpu.VMEM((GROUP1, block, block), f32),
            pltpu.VMEM((leaves, frame, block), f32),
            pltpu.VMEM((leaves, block, block), f32),
            pltpu.VMEM((frame, block), bf16),
            pltpu.VMEM((frame, block), bf16),
            pltpu.VMEM((block, frame), bf16),
            pltpu.VMEM((block, frame), bf16),
            pltpu.VMEM((NODES2, frame, block), f32),
            pltpu.VMEM((NODES2, block, block), f32),
            pltpu.VMEM((GROUP1, frame, block), f32),
            pltpu.VMEM((GROUP1, block, block), f32),
            pltpu.VMEM((leaves, frame, block), f32),
            pltpu.VMEM((leaves, block, block), f32),
            pltpu.SemaphoreType.DMA((GROUP2,)),
            pltpu.SemaphoreType.DMA((2, GROUP1)),
            pltpu.SemaphoreType.DMA((2,)),
            pltpu.SemaphoreType.DMA((6,)),
        ],
        compiler_params=pltpu.CompilerParams(vmem_limit_bytes=48 * 1024 * 1024),
        name="solve",
    )(*scalars, *arrays)


def body(
    root_frame,
    top_lhat,
    top_dinv,
    mid_lhat,
    mid_dinv,
    leaf_lhat,
    leaf_dinv,
    top_columns,
    mid_columns,
    leaf_columns,
    top_pattern,
    mid_parent,
    leaf_parent,
    mid_pattern,
    leaf_pattern,
    leaf_live,
):
    device = lax.axis_index("leaf").astype(jnp.int32)
    member = device % GROUP2
    block = top_dinv.shape[1]
    rows_root = BLOCKS * block // GROUP2
    if root_frame.shape[0] != rows_root:
        root_whole = lax.all_gather(root_frame, "leaf", axis=0, tiled=True)
        root_frame = lax.dynamic_slice_in_dim(root_whole, member * rows_root, rows_root, 0)
    row_block = member // GROUP1
    far = row_block // (BLOCKS // 2)
    right = (member % GROUP1 // (GROUP1 // 2)) ^ far
    own = pack(jnp.stack([row_block, right]), root_frame, top_lhat, top_dinv)

    across = exchange(own, 2)
    streams = [along_layers(own), None, along_layers(across), None]
    streams[1] = [exchange(x, 1) for x in streams[0]]
    streams[3] = [exchange(x, 1) for x in streams[2]]

    mid_own = (mid_lhat[0], mid_dinv[0])
    mid_across = tuple(exchange(x, 2) for x in mid_own)
    mids = [mid_own, tuple(exchange(x, 1) for x in mid_own), mid_across, None]
    mids[3] = tuple(exchange(x, 1) for x in mid_across)

    scalars = (
        device[None],
        top_columns,
        mid_columns,
        leaf_columns,
        top_pattern,
        mid_parent,
        leaf_parent,
        mid_pattern,
        leaf_pattern,
        leaf_live,
    )
    rows = (rows_root, top_lhat.shape[0], top_dinv.shape[0])
    top_diag, top_coup, mid_diag, mid_coup, leaf_diag, leaf_coup = solve_all(
        scalars, streams, mids, leaf_lhat, leaf_dinv, rows
    )
    return top_diag, top_coup, mid_diag[None], mid_coup[None], leaf_diag, leaf_coup


def solution(mesh):
    split_2 = P(("pole", "leaf"), None)
    split_3 = P(("pole", "leaf"), None, None)
    in_specs = (split_2,) * 3 + (split_3,) * 4 + (P(),) * 9
    out_specs = (split_2,) * 2 + (split_3,) * 4
    return jax.shard_map(body, mesh=mesh, in_specs=in_specs, out_specs=out_specs, check_vma=False)
```
